16 devices in a mesh: dp: 4 (over y, z, core), tp: 4 (over x).
Axes of the slice: x: 4, y: 2, z: 1, core: 2. Of those that a mesh axis runs over, the one named last changes fastest.
The devices are a block of a 4x4x8 slice.
Arguments:
- x: bfloat16 [3584, 5120], P(('dp', 'tp')), parts along dimension 0
- w_gate: bfloat16 [5120, 17408], P(None, 'tp')
- w_up: bfloat16 [5120, 17408], P(None, 'tp')
- w_down: bfloat16 [17408, 5120], P('tp')
Outputs:
- output: bfloat16 [3584, 5120], P(('dp', 'tp')), parts along dimension 0
There are 4 independent parts. The reference program is written for one: setup_inputs(seed, part) draws one part's arguments, and reference() takes and returns one part's arrays. A program takes and returns all parts, laid end to end along the dimension named above; an argument that names none is the same for every part.
All inputs are finite; a program needn't handle non-finite values.
Results may differ from the reference program's by a relative error of at most 0.016.
Values are sent between devices in bfloat16 or wider.
A program may use at most 768 MiB of HBM per device.

```python
import jax
import jax.numpy as jnp

ROWS = 896
D = 5120
FF = 17408


def setup_inputs(seed: int = 0, part: int = 0) -> dict:
    kx, kg, ku, kd = jax.random.split(jax.random.key(seed), 4)
    drawn = {
        "x": jax.random.normal(jax.random.fold_in(kx, part), (ROWS, D), jnp.float32),
        "w_gate": jax.random.normal(kg, (D, FF), jnp.float32) * D**-0.5,
        "w_up": jax.random.normal(ku, (D, FF), jnp.float32) * D**-0.5,
        "w_down": jax.random.normal(kd, (FF, D), jnp.float32) * FF**-0.5,
    }
    return {k: v.astype(jnp.bfloat16) for k, v in drawn.items()}


def reference(x, w_gate, w_up, w_down):
    gate = jnp.dot(x, w_gate, preferred_element_type=jnp.float32)
    up = jnp.dot(x, w_up, preferred_element_type=jnp.float32)
    hidden = (jax.nn.silu(gate) * up).astype(jnp.bfloat16)
    return jnp.dot(hidden, w_down, preferred_element_type=jnp.float32).astype(jnp.bfloat16)
```

```python
import functools

import jax
import jax.numpy as jnp
from jax import lax
from jax.experimental import pallas as pl
from jax.experimental.pallas import tpu as pltpu
from jax.sharding import PartitionSpec as P

BF = jnp.bfloat16
F32 = jnp.float32
MESH = pl.DeviceIdType.MESH
SLOTS = 4
TF = 256
TN = 512
CHUNK = (80, 80, 64)
PIECES = ((0, 0, 48), (0, 48, 32), (1, 0, 48), (1, 48, 32), (2, 0, 32), (2, 32, 32))
LEFT, RIGHT = 0, 1
DIAG, DIRECT, SUM = 0, 1, 2


def _kernel(
    x, wg, wu, wd, y,
    xown, xc, h, ring, ds, dg, st, rc, lsum, yown,
    xsem, wsem, ag_s, ag_r, fw_s, fw_r, rs_s, rs_r,
):
    rows, d = x.shape
    ff = wg.shape[1]
    half = d // 2
    n_gu = ff // TF
    pairs = half // TN
    n_dn = 2 * pairs
    start_row = [sum(CHUNK[:c]) for c in range(len(CHUNK))]
    top = 3 * max(CHUNK)

    me = lax.axis_index("tp")
    n = lax.axis_size("tp")
    peer = (lax.rem(me + n - 1, n), lax.rem(me + 1, n))

    def remote(src, dst, ssem, rsem, way):
        return pltpu.make_async_remote_copy(
            src_ref=src, dst_ref=dst, send_sem=ssem, recv_sem=rsem,
            device_id={"tp": peer[way]}, device_id_type=MESH,
        )

    def gu_copies(i, slot):
        cols = pl.ds(pl.multiple_of(i * TF, TF), TF)
        return (
            pltpu.make_async_copy(wg.at[:, cols], ring.at[slot, :, pl.ds(0, TF)], wsem.at[slot, 0]),
            pltpu.make_async_copy(wu.at[:, cols], ring.at[slot, :, pl.ds(TF, TF)], wsem.at[slot, 1]),
        )

    def dn_cols(t):
        return lax.rem(t, 2) * half + (t // 2) * TN

    def dn_copies(t, slot):
        cols = pl.ds(pl.multiple_of(dn_cols(t), TN), TN)
        return (pltpu.make_async_copy(wd.at[:, cols], ring.at[slot, pl.ds(0, ff), :], wsem.at[slot, 0]),)

    def fetch(kind, i, slot):
        for c in (gu_copies if kind == "gu" else dn_copies)(i, slot):
            c.start()

    def next_fetch(kind, count, nxt, i, slot):
        ahead = i + SLOTS - 1
        to = lax.rem(slot + SLOTS - 1, SLOTS)

        @pl.when(ahead < count)
        def _():
            fetch(kind, ahead, to)

        if nxt is not None:
            @pl.when(ahead >= count)
            def _():
                fetch(nxt, ahead - count, to)

    def own_piece(p, way):
        c, lo, m = PIECES[p]
        sec = 0 if way == RIGHT else CHUNK[c]
        return remote(
            xown.at[pl.ds(start_row[c] + lo, m), :], xc.at[c, pl.ds(sec + lo, m), :],
            ag_s.at[way, p], ag_r.at[way, p], way,
        )

    def fwd_piece(p, way):
        c, lo, m = PIECES[p]
        sec = 0 if way == RIGHT else CHUNK[c]
        cols = pl.ds(0 if way == RIGHT else half, half)
        return remote(
            xc.at[c, pl.ds(sec + lo, m), cols], xc.at[c, pl.ds(2 * CHUNK[c] + lo, m), cols],
            fw_s.at[way, p], fw_r.at[way, p], way,
        )

    def send_own(*ps):
        for p in ps:
            for way in (LEFT, RIGHT):
                own_piece(p, way).start()

    def forward(*ps):
        for p in ps:
            for way in (LEFT, RIGHT):
                own_piece(p, way).wait_recv()
                fwd_piece(p, way).start()

    def gathered(*ps):
        for p in ps:
            for way in (LEFT, RIGHT):
                fwd_piece(p, way).wait_recv()

    def hcol(j):
        return pl.ds(pl.multiple_of(j * TN, TN), TN)

    def acol(way, kind, j):
        first = (way == LEFT) == (kind != DIRECT)
        return pl.ds(pl.multiple_of((0 if first else half) + j * TN, TN), TN)

    def rs_copy(way, kind, c, j):
        r = pl.ds(start_row[c], CHUNK[c])
        if kind == DIAG:
            src, dst = ds.at[way, r, hcol(j)], dg.at[way, r, hcol(j)]
        else:
            cols = acol(way, kind, j)
            src, dst = st.at[way, r, cols], rc.at[way, r, cols]
        return remote(src, dst, rs_s.at[way, kind, c, j], rs_r.at[way, kind, c, j], way)

    def add_diag(c, j):
        m, r = CHUNK[c], pl.ds(start_row[c], CHUNK[c])
        for way in (LEFT, RIGHT):
            rs_copy(way, DIAG, c, j).wait_recv()
            total = lsum[way, pl.ds(0, m), hcol(j)] + dg[way, r, hcol(j)].astype(F32)
            st[way, r, acol(way, SUM, j)] = total.astype(BF)

    def send_sum(c, j):
        for way in (LEFT, RIGHT):
            rs_copy(way, SUM, c, j).start()

    def gate_up(lhs, m, h0, base, nxt, act):
        def body(i, carry):
            slot = lax.rem(base + i, SLOTS)
            for c in gu_copies(i, slot):
                c.wait()
            next_fetch("gu", n_gu, nxt, i, slot)
            act(i)
            acc = jnp.dot(lhs[pl.ds(0, m), :], ring[slot], preferred_element_type=F32)
            gate, up = acc[:, :TF], acc[:, TF:]
            h[pl.ds(h0, m), pl.ds(pl.multiple_of(i * TF, TF), TF)] = (jax.nn.silu(gate) * up).astype(BF)
            return carry

        lax.fori_loop(0, n_gu, body, 0)

    def down(c, h0, base, nxt, own, before, after):
        m = CHUNK[c]
        r = pl.ds(start_row[c], m)
        total = 3 * m + (rows if own else 0)

        def tile(j, which):
            t = 2 * j + which
            slot = lax.rem(base + t, SLOTS)
            for cp in dn_copies(t, slot):
                cp.wait()
            next_fetch("dn", n_dn, nxt, t, slot)
            return slot

        def product(slot, j, which):
            acc = jnp.dot(h[pl.ds(h0, total), :], ring[slot, pl.ds(0, ff), :], preferred_element_type=F32)
            diag_way = LEFT if which == 0 else RIGHT
            sec = (acc[0:m], acc[m:2 * m])
            ds[diag_way, r, hcol(j)] = acc[2 * m:3 * m].astype(BF)
            lsum[diag_way, pl.ds(0, m), hcol(j)] = sec[diag_way]
            st[1 - diag_way, r, acol(1 - diag_way, DIRECT, j)] = sec[1 - diag_way].astype(BF)
            if own:
                yown[:, pl.ds(pl.multiple_of(which * half + j * TN, TN), TN)] = acc[3 * m:]

        def send(j, which):
            diag_way = LEFT if which == 0 else RIGHT
            rs_copy(diag_way, DIAG, c, j).start()
            rs_copy(1 - diag_way, DIRECT, c, j).start()

        def body(j, carry):
            slot = tile(j, 0)

            @pl.when(j > 0)
            def _():
                send(j - 1, 1)

            before(j)
            product(slot, j, 0)
            slot = tile(j, 1)
            send(j, 0)
            after(j)
            product(slot, j, 1)
            return carry

        lax.fori_loop(0, pairs, body, 0)
        send(pairs - 1, 1)

    load = pltpu.make_async_copy(x, xown, xsem)
    load.start()
    for s in range(SLOTS - 1):
        fetch("gu", s, s)
    barrier = pltpu.get_barrier_semaphore()
    for way in (LEFT, RIGHT):
        pl.semaphore_signal(barrier, inc=1, device_id={"tp": peer[way]}, device_id_type=MESH)
    load.wait()
    pl.semaphore_wait(barrier, 2)
    send_own(0, 1)

    def act0(i):
        @pl.when(i == 9)
        def _():
            forward(0)

        @pl.when(i == 14)
        def _():
            forward(1)
            send_own(2, 3)

    gate_up(xown, rows, top, 0, "gu", act0)
    base = n_gu
    gathered(0, 1)

    def act1(i):
        @pl.when(i == 6)
        def _():
            forward(2)

        @pl.when(i == 11)
        def _():
            forward(3)
            send_own(4, 5)

    def sums(c, first):
        def act(i):
            k = i - first

            @pl.when((k >= 0) & (k < 2 * pairs))
            def _():
                @pl.when(lax.rem(k, 2) == 0)
                def _():
                    add_diag(c, k // 2)

                @pl.when(lax.rem(k, 2) == 1)
                def _():
                    send_sum(c, k // 2)

        return act

    sums0, sums1 = sums(0, 6), sums(1, 2)

    def act2(i):
        @pl.when(i == 1)
        def _():
            forward(4, 5)

        sums0(i)

    none = lambda j: None
    gate_up(xc.at[0], 3 * CHUNK[0], top - 3 * CHUNK[0], base, "dn", act1)
    base += n_gu
    down(0, top - 3 * CHUNK[0], base, "gu", False, none, none)
    base += n_dn
    gathered(2, 3)
    gate_up(xc.at[1], 3 * CHUNK[1], top - 3 * CHUNK[1], base, "dn", act2)
    base += n_gu
    down(1, top - 3 * CHUNK[1], base, "gu", False, none, none)
    base += n_dn
    gathered(4, 5)
    gate_up(xc.at[2], 3 * CHUNK[2], top - 3 * CHUNK[2], base, "dn", sums1)
    base += n_gu

    lag = 2

    def tail_add(j):
        @pl.when(j >= lag)
        def _():
            add_diag(2, j - lag)

    def tail_send(j):
        @pl.when(j >= lag)
        def _():
            send_sum(2, j - lag)

    down(2, top - 3 * CHUNK[2], base, None, True, tail_add, tail_send)

    def finish(j):
        for which in (0, 1):
            cols = pl.ds(pl.multiple_of(which * half + j * TN, TN), TN)
            for way in (LEFT, RIGHT):
                kind = SUM if (way == LEFT) == (which == 0) else DIRECT
                for c in range(len(CHUNK)):
                    rs_copy(way, kind, c, j).wait_recv()
            y[:, cols] = (yown[:, cols] + rc[LEFT, :, cols].astype(F32) + rc[RIGHT, :, cols].astype(F32)).astype(BF)

    def last_sums(j, carry):
        add_diag(2, j)
        finish(j - (pairs - lag))
        send_sum(2, j)
        return carry

    lax.fori_loop(pairs - lag, pairs, last_sums, 0)

    def finish_all(j, carry):
        finish(j)
        return carry

    lax.fori_loop(lag, pairs, finish_all, 0)

    for p in range(len(PIECES)):
        for way in (LEFT, RIGHT):
            own_piece(p, way).wait_send()
            fwd_piece(p, way).wait_send()
    for c in range(len(CHUNK)):
        def drain(j, carry, c=c):
            for way in (LEFT, RIGHT):
                for kind in (DIAG, DIRECT, SUM):
                    rs_copy(way, kind, c, j).wait_send()
            return carry

        lax.fori_loop(0, pairs, drain, 0)


def solution(mesh):
    def step(x, w_gate, w_up, w_down):
        rows, d = x.shape
        ff = w_gate.shape[1]
        half, pairs = d // 2, d // 2 // TN
        top = 3 * max(CHUNK)
        any_spec = pl.BlockSpec(memory_space=pl.ANY)
        dma = pltpu.SemaphoreType.DMA
        return pl.pallas_call(
            _kernel,
            out_shape=jax.ShapeDtypeStruct((rows, d), BF),
            in_specs=[any_spec] * 4,
            out_specs=pl.BlockSpec(memory_space=pltpu.VMEM),
            scratch_shapes=[
                pltpu.VMEM((rows, d), BF),
                pltpu.VMEM((len(CHUNK), top, d), BF),
                pltpu.VMEM((top + rows, ff), BF),
                pltpu.VMEM((SLOTS, d, max(2 * TF, TN)), BF),
                pltpu.VMEM((2, rows, half), BF),
                pltpu.VMEM((2, rows, half), BF),
                pltpu.VMEM((2, rows, d), BF),
                pltpu.VMEM((2, rows, d), BF),
                pltpu.VMEM((2, max(CHUNK), half), F32),
                pltpu.VMEM((rows, d), F32),
                dma(()),
                dma((SLOTS, 2)),
                dma((2, len(PIECES))),
                dma((2, len(PIECES))),
                dma((2, len(PIECES))),
                dma((2, len(PIECES))),
                dma((2, 3, len(CHUNK), pairs)),
                dma((2, 3, len(CHUNK), pairs)),
            ],
            compiler_params=pltpu.CompilerParams(
                collective_id=0, has_side_effects=True, vmem_limit_bytes=67_043_328
            ),
            cost_estimate=pl.CostEstimate(
                flops=6 * 4 * rows * d * ff, bytes_accessed=4 * 6 * d * ff, transcendentals=4 * rows * ff
            ),
        )(x, w_gate, w_up, w_down)

    return jax.shard_map(
        step,
        mesh=mesh,
        in_specs=(P(("dp", "tp"), None), P(None, "tp"), P(None, "tp"), P("tp", None)),
        out_specs=P(("dp", "tp"), None),
        check_vma=False,
    )
```

```python
import functools

import jax
import jax.numpy as jnp
from jax import lax
from jax.experimental import pallas as pl
from jax.experimental.pallas import tpu as pltpu
from jax.sharding import PartitionSpec as P

BF = jnp.bfloat16
F32 = jnp.float32
MESH = pl.DeviceIdType.MESH
SLOTS = 6
TF = 256
TN = 512
CHUNK = (64, 96, 64)
PIECES = ((0, 0, 32), (0, 32, 32), (1, 0, 48), (1, 48, 48), (2, 0, 32), (2, 32, 32))
LEFT, RIGHT = 0, 1
DIAG, DIRECT, SUM = 0, 1, 2


def _kernel(
    x, wg, wu, wd, y,
    xown, xc, h, ring, ds, dg, st, rc, lsum, yown,
    xsem, wsem, ag_s, ag_r, fw_s, fw_r, rs_s, rs_r,
):
    rows, d = x.shape
    ff = wg.shape[1]
    half = d // 2
    n_gu = ff // TF
    pairs = half // TN
    n_dn = 2 * pairs
    start_row = [sum(CHUNK[:c]) for c in range(len(CHUNK))]
    top = 3 * max(CHUNK)

    me = lax.axis_index("tp")
    n = lax.axis_size("tp")
    peer = (lax.rem(me + n - 1, n), lax.rem(me + 1, n))

    def remote(src, dst, ssem, rsem, way):
        return pltpu.make_async_remote_copy(
            src_ref=src, dst_ref=dst, send_sem=ssem, recv_sem=rsem,
            device_id={"tp": peer[way]}, device_id_type=MESH,
        )

    def gu_copies(i, slot):
        cols = pl.ds(pl.multiple_of(i * TF, TF), TF)
        return (
            pltpu.make_async_copy(wg.at[:, cols], ring.at[slot, :, pl.ds(0, TF)], wsem.at[slot, 0]),
            pltpu.make_async_copy(wu.at[:, cols], ring.at[slot, :, pl.ds(TF, TF)], wsem.at[slot, 1]),
        )

    def dn_cols(t):
        return lax.rem(t, 2) * half + (t // 2) * TN

    def dn_copies(t, slot):
        cols = pl.ds(pl.multiple_of(dn_cols(t), TN), TN)
        return (pltpu.make_async_copy(wd.at[:, cols], ring.at[slot, pl.ds(0, ff), :], wsem.at[slot, 0]),)

    far = 100 * SLOTS + n_gu - 1

    def slot_up(q):
        return lax.rem(q, SLOTS)

    def slot_down(q):
        return lax.rem(far - q, SLOTS)

    def fetch(kind, i, slot):
        for c in (gu_copies if kind != "dn" else dn_copies)(n_gu - 1 - i if kind == "ug" else i, slot):
            c.start()

    def arrive(kind, i, slot):
        for c in (gu_copies if kind != "dn" else dn_copies)(n_gu - 1 - i if kind == "ug" else i, slot):
            c.wait()

    def fetch_ahead(kind, count, nxt, i, base, slot_of):
        if isinstance(i, int):
            if i < count:
                fetch(kind, i, slot_of(base + i))
            elif nxt is not None:
                fetch(nxt, i - count, slot_of(base + i))
            return

        @pl.when(i < count)
        def _():
            fetch(kind, i, slot_of(base + i))

        if nxt is not None:
            @pl.when(i >= count)
            def _():
                fetch(nxt, i - count, slot_of(base + i))

    def own_piece(p, way):
        c, lo, m = PIECES[p]
        sec = 0 if way == RIGHT else CHUNK[c]
        return remote(
            x.at[pl.ds(start_row[c] + lo, m), :], xc.at[pl.ds(3 * start_row[c] + sec + lo, m), :],
            ag_s.at[way, p], ag_r.at[way, p], way,
        )

    def fwd_piece(p, way):
        c, lo, m = PIECES[p]
        sec = 0 if way == RIGHT else CHUNK[c]
        cols = pl.ds(0 if way == RIGHT else half, half)
        return remote(
            xc.at[pl.ds(3 * start_row[c] + sec + lo, m), cols],
            xc.at[pl.ds(3 * start_row[c] + 2 * CHUNK[c] + lo, m), cols],
            fw_s.at[way, p], fw_r.at[way, p], way,
        )

    def send_own(*ps):
        for p in ps:
            for way in (LEFT, RIGHT):
                own_piece(p, way).start()

    def forward(*ps):
        for p in ps:
            for way in (LEFT, RIGHT):
                own_piece(p, way).wait_recv()
                fwd_piece(p, way).start()

    def gathered(*ps):
        for p in ps:
            for way in (LEFT, RIGHT):
                fwd_piece(p, way).wait_recv()

    def hcol(j):
        return pl.ds(pl.multiple_of(j * TN, TN), TN)

    def acol(way, kind, j):
        first = (way == LEFT) == (kind != DIRECT)
        return pl.ds(pl.multiple_of((0 if first else half) + j * TN, TN), TN)

    def rs_copy(way, kind, c, j):
        r = pl.ds(start_row[c], CHUNK[c])
        if kind == DIAG:
            src, dst = ds.at[way, r, hcol(j)], dg.at[way, r, hcol(j)]
        else:
            cols = acol(way, kind, j)
            src, dst = st.at[way, r, cols], rc.at[way, r, cols]
        return remote(src, dst, rs_s.at[way, kind, c, j], rs_r.at[way, kind, c, j], way)

    def add_diag(c, j):
        m, r = CHUNK[c], pl.ds(start_row[c], CHUNK[c])
        for way in (LEFT, RIGHT):
            rs_copy(way, DIAG, c, j).wait_recv()
            total = lsum[way, pl.ds(0, m), hcol(j)] + dg[way, r, hcol(j)].astype(F32)
            st[way, r, acol(way, SUM, j)] = total.astype(BF)

    def send_sum(c, j):
        for way in (LEFT, RIGHT):
            rs_copy(way, SUM, c, j).start()

    def gate_up(lhs, r0, m, h0, kind, base, slot_of, nxt, act, after_pair=False):
        def body(i, carry):
            slot = slot_of(base + i)
            if kind == "ug":
                @pl.when(i >= SLOTS)
                def _():
                    arrive(kind, i, slot)

                @pl.when(i >= 1)
                def _():
                    fetch_ahead(kind, n_gu, nxt, i + SLOTS - 1, base, slot_of)
            else:
                arrive(kind, i, slot)
                if after_pair:
                    @pl.when(i == 0)
                    def _():
                        fetch(kind, SLOTS - 2, slot_of(base + SLOTS - 2))
                fetch_ahead(kind, n_gu, nxt, i + SLOTS - 1, base, slot_of)
            act(i)
            hidden(lhs, r0, m, h0, kind, i, slot)
            return carry

        lax.fori_loop(0, n_gu, body, 0)

    def hidden(lhs, r0, m, h0, kind, i, slot):
        acc = jnp.dot(lhs[pl.ds(r0, m), :], ring[slot], preferred_element_type=F32)
        gate, up = acc[:, :TF], acc[:, TF:]
        tile = n_gu - 1 - i if kind == "ug" else i
        cols = pl.ds(tile * TF if isinstance(tile, int) else pl.multiple_of(tile * TF, TF), TF)
        h[pl.ds(h0, m), cols] = (jax.nn.silu(gate) * up).astype(BF)

    def gate_up_pairs(lhs, r0, m, h0, base, nxt, act):
        def body(k, carry):
            i = 2 * k
            for w in (0, 1):
                arrive("gu", i + w, slot_down(base + i + w))

            @pl.when(k > 0)
            def _():
                fetch_ahead("gu", n_gu, nxt, i + SLOTS - 2, base, slot_down)

            fetch_ahead("gu", n_gu, nxt, i + SLOTS - 1, base, slot_down)
            act(k)
            for w in (0, 1):
                hidden(lhs, r0, m, h0, "gu", i + w, slot_down(base + i + w))
            return carry

        lax.fori_loop(0, n_gu // 2, body, 0)
        i = n_gu - 1
        arrive("gu", i, slot_down(base + i))
        for a in (SLOTS - 2, SLOTS - 1):
            fetch_ahead("gu", n_gu, nxt, i + a, base, slot_down)
        hidden(lhs, r0, m, h0, "gu", i, slot_down(base + i))

    def kind_of(way, which):
        return SUM if (way == LEFT) == (which == 0) else DIRECT

    def terms(c, acc, j, which):
        m = CHUNK[c]
        r = pl.ds(start_row[c], m)
        diag_way = LEFT if which == 0 else RIGHT
        sec = (acc[0:m], acc[m:2 * m])
        ds[diag_way, r, hcol(j)] = acc[2 * m:3 * m].astype(BF)
        lsum[diag_way, pl.ds(0, m), hcol(j)] = sec[diag_way]
        st[1 - diag_way, r, acol(1 - diag_way, DIRECT, j)] = sec[1 - diag_way].astype(BF)

    def own_rows(acc, j, which):
        cols = pl.ds(pl.multiple_of(which * half + j * TN, TN), TN)
        early = rows - CHUNK[-1]
        for c in range(len(CHUNK) - 1):
            for way in (LEFT, RIGHT):
                rs_copy(way, kind_of(way, which), c, j).wait_recv()
        y[pl.ds(0, early), cols] = (
            acc[:early]
            + rc[LEFT, pl.ds(0, early), cols].astype(F32)
            + rc[RIGHT, pl.ds(0, early), cols].astype(F32)
        ).astype(BF)
        yown[:, cols] = acc[early:]

    def product(slot, r0, m):
        return jnp.dot(h[pl.ds(r0, m), :], ring[slot, pl.ds(0, ff), :], preferred_element_type=F32)

    def send_terms(c, j, which):
        diag_way = LEFT if which == 0 else RIGHT
        rs_copy(diag_way, DIAG, c, j).start()
        rs_copy(1 - diag_way, DIRECT, c, j).start()

    def down(c, base, nxt, act):
        def body(j, carry):
            for w in (0, 1):
                t = 2 * j + w
                slot = slot_down(base + t)
                arrive("dn", t, slot)
                fetch_ahead("dn", n_dn, nxt, t + SLOTS - 1, base, slot_down)
                if w == 1:
                    send_terms(c, j, 0)
                else:
                    @pl.when(j > 0)
                    def _():
                        send_terms(c, j - 1, 1)
                    act(j)
                terms(c, product(slot, h0[c], 3 * CHUNK[c]), j, w)
            return carry

        lax.fori_loop(0, pairs, body, 0)
        send_terms(c, pairs - 1, 1)

    def down_pairs(c, base, nxt):
        def body(j, carry):
            t = 2 * j
            slots = [slot_down(base + t + w) for w in (0, 1)]
            for w in (0, 1):
                arrive("dn", t + w, slots[w])

            @pl.when(j > 0)
            def _():
                fetch_ahead("dn", n_dn, nxt, t + SLOTS - 2, base, slot_down)

            fetch_ahead("dn", n_dn, nxt, t + SLOTS - 1, base, slot_down)

            @pl.when(j > 0)
            def _():
                for w in (0, 1):
                    send_terms(c, j - 1, w)

            for w in (0, 1):
                terms(c, product(slots[w], h0[c], 3 * CHUNK[c]), j, w)
            return carry

        lax.fori_loop(0, pairs, body, 0)
        for w in (0, 1):
            send_terms(c, pairs - 1, w)

    def down_last(c, base):
        def tile(t):
            slot = slot_down(base + t)
            arrive("dn", t, slot)

            @pl.when(t + SLOTS - 1 < n_dn)
            def _():
                fetch("dn", t + SLOTS - 1, slot_down(base + t + SLOTS - 1))

            return slot

        m3 = 3 * CHUNK[c]

        def both(j, carry):
            for w in (0, 1):
                slot = tile(2 * j + w)
                if w == 1:
                    send_terms(c, j, 0)

                    @pl.when(j >= lag)
                    def _():
                        send_sum(c, j - lag)
                else:
                    @pl.when(j > 0)
                    def _():
                        send_terms(c, j - 1, 1)

                    @pl.when(j >= lag)
                    def _():
                        add_diag(c, j - lag)
                acc = product(slot, h0[c], m3 + rows)
                terms(c, acc[:m3], j, w)
                own_rows(acc[m3:], j, w)
            return carry

        def peers(j, carry):
            for w in (0, 1):
                slot = tile(2 * j + w)
                if w == 1:
                    send_terms(c, j, 0)
                    send_sum(c, j - lag)
                else:
                    send_terms(c, j - 1, 1)
                    add_diag(c, j - lag)
                terms(c, product(slot, h0[c], m3), j, w)
            return carry

        def mine(j, carry):
            for w in (0, 1):
                if w == 1:
                    @pl.when(j == split)
                    def _():
                        add_diag(c, split)
                else:
                    @pl.when(j == split)
                    def _():
                        send_terms(c, pairs - 1, 1)

                    @pl.when(j > split)
                    def _():
                        send_sum(c, split)
                own_rows(product(slot_down(base + 2 * j + w), top, rows), j, w)
            return carry

        split = pairs - lag
        lax.fori_loop(0, split, both, 0)
        lax.fori_loop(split, pairs, peers, 0)
        lax.fori_loop(split, pairs, mine, 0)

    h0 = [top - 3 * m for m in CHUNK]
    lag = 2

    barrier = pltpu.get_barrier_semaphore()
    for way in (LEFT, RIGHT):
        pl.semaphore_signal(barrier, inc=1, device_id={"tp": peer[way]}, device_id_type=MESH)
    load = pltpu.make_async_copy(x, xown, xsem)
    load.start()
    fetch("gu", 0, slot_up(0))
    pl.semaphore_wait(barrier, 2)
    send_own(0)
    load.wait()
    for i in range(1, SLOTS - 1):
        fetch("gu", i, slot_up(i))

    def at(step, i, *do):
        @pl.when(i == step)
        def _():
            for f, ps in do:
                f(*ps)

    def act0(i):
        at(3, i, (send_own, (1,)))
        at(7, i, (forward, (0,)))
        at(11, i, (forward, (1,)))
        at(13, i, (send_own, (2,)))

    gate_up(xown, 0, rows, top, "gu", 0, slot_up, None, act0)
    gathered(0, 1)

    def act1(i):
        at(3, i, (send_own, (3,)))
        at(8, i, (forward, (2,)))

    def act1d(j):
        at(0, j, (forward, (3,)))

    def sums(c, first):
        def act(k):
            @pl.when((k > first) & (k <= first + pairs))
            def _():
                send_sum(c, k - first - 1)

            @pl.when((k >= first) & (k < first + pairs))
            def _():
                add_diag(c, k - first)

        return act

    def drain_gather():
        for p in range(len(PIECES)):
            for way in (LEFT, RIGHT):
                own_piece(p, way).wait_send()
                fwd_piece(p, way).wait_send()

    def drain_terms(c):
        def body(j, carry):
            for way in (LEFT, RIGHT):
                for kind in (DIAG, DIRECT, SUM):
                    rs_copy(way, kind, c, j).wait_send()
            return carry

        lax.fori_loop(0, pairs, body, 0)

    sums0 = sums(0, 2)

    def act2(k):
        at(0, k, (send_own, (4, 5)))
        at(7, k, (forward, (4, 5)))
        sums0(k)

    def act3(i):
        k = i - 2

        @pl.when((k >= 0) & (k < 2 * pairs))
        def _():
            @pl.when(lax.rem(k, 2) == 0)
            def _():
                add_diag(1, k // 2)

            @pl.when(lax.rem(k, 2) == 1)
            def _():
                send_sum(1, k // 2)

        at(13, i, (drain_gather, ()))
        at(14, i, (drain_terms, (0,)))

    base = 0
    gate_up(xc, 0, 3 * CHUNK[0], h0[0], "ug", base, slot_down, "dn", act1)
    base += n_gu
    down(0, base, "gu", act1d)
    base += n_dn
    gathered(2, 3)
    gate_up_pairs(xc, 3 * start_row[1], 3 * CHUNK[1], h0[1], base, "dn", act2)
    base += n_gu
    down_pairs(1, base, "gu")
    base += n_dn
    gathered(4, 5)
    gate_up(xc, 3 * start_row[2], 3 * CHUNK[2], h0[2], "gu", base, slot_down, "dn", act3, after_pair=True)
    base += n_gu
    down_last(2, base)

    last = pl.ds(start_row[2], CHUNK[2])

    def finish(j):
        for which in (0, 1):
            cols = pl.ds(pl.multiple_of(which * half + j * TN, TN), TN)
            for way in (LEFT, RIGHT):
                rs_copy(way, kind_of(way, which), 2, j).wait_recv()
            y[last, cols] = (
                yown[:, cols] + rc[LEFT, last, cols].astype(F32) + rc[RIGHT, last, cols].astype(F32)
            ).astype(BF)

    add_diag(2, pairs - 1)
    for j in range(lag):
        finish(j)
    send_sum(2, pairs - 1)
    drain_terms(1)

    def finish_all(j, carry):
        finish(j)
        return carry

    lax.fori_loop(lag, pairs, finish_all, 0)
    drain_terms(2)


def solution(mesh):
    def step(x, w_gate, w_up, w_down):
        rows, d = x.shape
        ff = w_gate.shape[1]
        half, pairs = d // 2, d // 2 // TN
        top = 3 * max(CHUNK)
        any_spec = pl.BlockSpec(memory_space=pl.ANY)
        dma = pltpu.SemaphoreType.DMA
        return pl.pallas_call(
            _kernel,
            out_shape=pltpu.VMEM((rows, d), BF),
            in_specs=[any_spec] * 4,
            out_specs=pl.BlockSpec(memory_space=pltpu.VMEM),
            scratch_shapes=[
                pltpu.VMEM((rows, d), BF),
                pltpu.VMEM((3 * rows, d), BF),
                pltpu.VMEM((top + rows, ff), BF),
                pltpu.VMEM((SLOTS, d, max(2 * TF, TN)), BF),
                pltpu.VMEM((2, rows, half), BF),
                pltpu.VMEM((2, rows, half), BF),
                pltpu.VMEM((2, rows, d), BF),
                pltpu.VMEM((2, rows, d), BF),
                pltpu.VMEM((2, max(CHUNK), half), F32),
                pltpu.VMEM((CHUNK[-1], d), F32),
                dma(()),
                dma((SLOTS, 2)),
                dma((2, len(PIECES))),
                dma((2, len(PIECES))),
                dma((2, len(PIECES))),
                dma((2, len(PIECES))),
                dma((2, 3, len(CHUNK), pairs)),
                dma((2, 3, len(CHUNK), pairs)),
            ],
            compiler_params=pltpu.CompilerParams(
                collective_id=0, has_side_effects=True, vmem_limit_bytes=64_600_000
            ),
            cost_estimate=pl.CostEstimate(
                flops=6 * 4 * rows * d * ff, bytes_accessed=4 * 6 * d * ff, transcendentals=4 * rows * ff
            ),
        )(x, w_gate, w_up, w_down)

    return jax.shard_map(
        step,
        mesh=mesh,
        in_specs=(P(("dp", "tp"), None), P(None, "tp"), P(None, "tp"), P("tp", None)),
        out_specs=P(("dp", "tp"), None),
        check_vma=False,
    )
```

```python
import jax
import jax.numpy as jnp
from jax import lax
from jax.experimental import pallas as pl
from jax.experimental.pallas import tpu as pltpu
from jax.sharding import PartitionSpec as P

BF = jnp.bfloat16
F32 = jnp.float32
MESH = pl.DeviceIdType.MESH
SLOTS = 6
TF = 256
TN = 512
CHUNK = (64, 80, 80)
PIECES = ((0, 0, 32), (0, 32, 32), (1, 0, 48), (1, 48, 32), (2, 0, 48), (2, 48, 32))
PART = ((0, CHUNK[0] + CHUNK[1]), (CHUNK[0] + CHUNK[1], CHUNK[2]))
LEFT, RIGHT = 0, 1
DIAG, DIRECT, SUM = 0, 1, 2


def _kernel(
    x, wg, wu, wd, y,
    xown, xc, h, ring, ds, st, rc, lsum, yown,
    xsem, wsem, ag_s, ag_r, fw_r, rs_s, dg_r, rc_r,
):
    rows, d = x.shape
    ff = wg.shape[1]
    half = d // 2
    n_gu = ff // TF
    pairs = half // TN
    n_dn = 2 * pairs
    start_row = [sum(CHUNK[:c]) for c in range(len(CHUNK))]
    top = 3 * PART[0][1]

    me = lax.axis_index("tp")
    n = lax.axis_size("tp")
    peer = (lax.rem(me + n - 1, n), lax.rem(me + 1, n))

    def remote(src, dst, ssem, rsem, way):
        return pltpu.make_async_remote_copy(
            src_ref=src, dst_ref=dst, send_sem=ssem, recv_sem=rsem,
            device_id={"tp": peer[way]}, device_id_type=MESH,
        )

    def gu_copies(i, slot):
        cols = pl.ds(pl.multiple_of(i * TF, TF), TF)
        return (
            pltpu.make_async_copy(wg.at[:, cols], ring.at[slot, :, pl.ds(0, TF)], wsem.at[slot]),
            pltpu.make_async_copy(wu.at[:, cols], ring.at[slot, :, pl.ds(TF, TF)], wsem.at[slot]),
        )

    def dn_copies(t, slot):
        start = t % 2 * half + t // 2 * TN if isinstance(t, int) else lax.rem(t, 2) * half + t // 2 * TN
        cols = pl.ds(start if isinstance(start, int) else pl.multiple_of(start, TN), TN)
        return (pltpu.make_async_copy(wd.at[:, cols], ring.at[slot, pl.ds(0, ff), :], wsem.at[slot]),)

    def slot_up(q):
        return lax.rem(q, SLOTS)

    def slot_back(q):
        return lax.rem(100 * SLOTS + n_gu - 1 - q, SLOTS)

    def copies(kind, i, slot):
        if kind == "dn":
            return dn_copies(i, slot)
        return gu_copies(n_gu - 1 - i if kind == "ug" else i, slot)

    def fetch(kind, i, slot):
        for c in copies(kind, i, slot):
            c.start()

    def arrive(kind, i, slot):
        if kind == "dn":
            got = dn_copies(i, slot)
        else:
            got = (pltpu.make_async_copy(wg.at[:, pl.ds(0, 2 * TF)], ring.at[slot], wsem.at[slot]),)
        for c in got:
            c.wait()

    def fetch_ahead(kind, count, nxt, i, base, slot_of):
        if isinstance(i, int):
            if i < count:
                fetch(kind, i, slot_of(base + i))
            elif nxt is not None:
                fetch(nxt, i - count, slot_of(base + i))
            return

        @pl.when(i < count)
        def _():
            fetch(kind, i, slot_of(base + i))

        if nxt is not None:
            @pl.when(i >= count)
            def _():
                fetch(nxt, i - count, slot_of(base + i))

    def own_piece(p, way):
        c, lo, m = PIECES[p]
        sec = 3 * start_row[c] + (0 if way == RIGHT else CHUNK[c]) + lo
        src = x.at[pl.ds(start_row[c] + lo, m), :]
        return remote(src, xc.at[pl.ds(sec, m), :], ag_s.at[way], ag_r.at[way, p], way)

    def fwd_copy(c, lo, m, way):
        sec = 3 * start_row[c] + (0 if way == RIGHT else CHUNK[c]) + lo
        to = 3 * start_row[c] + 2 * CHUNK[c] + lo
        cols = pl.ds(0 if way == RIGHT else half, half)
        return remote(xc.at[pl.ds(sec, m), cols], xc.at[pl.ds(to, m), cols], ag_s.at[way], fw_r.at[way, c], way)

    def send_own(*ps):
        for p in ps:
            for way in (LEFT, RIGHT):
                own_piece(p, way).start()

    def forward(*ps):
        for p in ps:
            for way in (LEFT, RIGHT):
                own_piece(p, way).wait_recv()
                fwd_copy(*PIECES[p], way).start()

    def gathered(c):
        for way in (LEFT, RIGHT):
            fwd_copy(c, 0, CHUNK[c], way).wait_recv()

    def drain(sem, m, way):
        remote(xc.at[pl.ds(0, m), :], xc.at[pl.ds(0, m), :], sem, ag_r.at[way, 0], way).wait_send()

    def col(which, j):
        start = which * half + j * TN
        return pl.ds(start if isinstance(start, int) else pl.multiple_of(start, TN), TN)

    def diag_copy(way, part, j, span=None):
        r = pl.ds(*(span or PART[part]))
        return remote(
            ds.at[r, col(way, j)], xown.at[r, col(way, j)], rs_s.at[way, part], dg_r.at[way, part, j], way
        )

    def term_copy(way, which, part, j, span=None):
        r = pl.ds(*(span or PART[part]))
        return remote(
            st.at[way, r, col(which, j)], rc.at[way, r, col(which, j)],
            rs_s.at[way, part], rc_r.at[way, j if part else pairs], way,
        )

    def add_diag(part, j):
        lo, m = PART[part]
        r = pl.ds(lo, m)
        for way in (LEFT, RIGHT):
            diag_copy(way, part, j).wait_recv()
            total = lsum[pl.ds(0, m), col(way, j)] + xown[r, col(way, j)].astype(F32)
            st[way, r, col(way, j)] = total.astype(BF)

    def send_sum(part, j):
        for way in (LEFT, RIGHT):
            term_copy(way, way, part, j).start()

    def send_terms(part, j, which, span=None):
        diag_copy(which, part, j, span).start()
        term_copy(1 - which, which, part, j, span).start()

    def terms(acc, part, lo, m, j, which):
        r = pl.ds(PART[part][0] + lo, m)
        sec = (acc[0:m], acc[m:2 * m])
        ds[r, col(which, j)] = acc[2 * m:3 * m].astype(BF)
        lsum[pl.ds(lo, m), col(which, j)] = sec[which]
        st[1 - which, r, col(which, j)] = sec[1 - which].astype(BF)

    def reduced(part, way, width, j):
        r, cols = pl.ds(*PART[part]), pl.ds(0, width)
        remote(st.at[way, r, cols], rc.at[way, r, cols], rs_s.at[way, part], rc_r.at[way, j], way).wait_recv()

    def own_rows(acc, j, which):
        r = pl.ds(*PART[0])
        m = PART[0][1]
        cols = col(which, j)
        y[r, cols] = (acc[:m] + rc[LEFT, r, cols].astype(F32) + rc[RIGHT, r, cols].astype(F32)).astype(BF)
        yown[:, cols] = acc[m:]

    def finish(j):
        r = pl.ds(*PART[1])
        for way in (LEFT, RIGHT):
            reduced(1, way, 2 * TN, j)
        for which in (0, 1):
            cols = col(which, j)
            y[r, cols] = (yown[:, cols] + rc[LEFT, r, cols].astype(F32) + rc[RIGHT, r, cols].astype(F32)).astype(BF)

    def hidden(lhs, r0, m, h0, tile, slot):
        acc = jnp.dot(lhs[pl.ds(r0, m), :], ring[slot], preferred_element_type=F32)
        gate, up = acc[:, :TF], acc[:, TF:]
        cols = pl.ds(tile * TF if isinstance(tile, int) else pl.multiple_of(tile * TF, TF), TF)
        h[pl.ds(h0, m), cols] = (jax.nn.silu(gate) * up).astype(BF)

    def product(slot, r0, m):
        return jnp.dot(h[pl.ds(r0, m), :], ring[slot, pl.ds(0, ff), :], preferred_element_type=F32)

    def gate_up(lhs, r0, m, h0, act):
        def body(i, carry):
            slot = slot_up(i)
            arrive("gu", i, slot)
            fetch_ahead("gu", n_gu, None, i + SLOTS - 1, 0, slot_up)
            act(i)
            hidden(lhs, r0, m, h0, i, slot)
            return carry

        lax.fori_loop(0, n_gu, body, 0)

    def gate_up_pairs(lhs, c, h0, kind, base, slot_of, nxt, act, resident):
        r0, m = 3 * start_row[c], 3 * CHUNK[c]
        tile_of = lambda i: n_gu - 1 - i if kind == "ug" else i

        def body(k, carry):
            i = 2 * k

            def wait():
                for w in (0, 1):
                    arrive(kind, i + w, slot_of(base + i + w))

            if resident:
                pl.when(i >= SLOTS)(wait)
            else:
                wait()

            @pl.when(k > 0)
            def _():
                for a in (SLOTS - 2, SLOTS - 1):
                    fetch_ahead(kind, n_gu, nxt, i + a, base, slot_of)

            if not resident:
                @pl.when(k == 0)
                def _():
                    fetch(kind, SLOTS - 1, slot_of(base + SLOTS - 1))

            act(k)
            for w in (0, 1):
                hidden(lhs, r0, m, h0, tile_of(i + w), slot_of(base + i + w))
            return carry

        lax.fori_loop(0, n_gu // 2, body, 0)
        i = n_gu - 1
        arrive(kind, i, slot_of(base + i))
        for a in (SLOTS - 2, SLOTS - 1):
            fetch_ahead(kind, n_gu, nxt, i + a, base, slot_of)
        act(n_gu // 2)
        hidden(lhs, r0, m, h0, tile_of(i), slot_of(base + i))

    def down_first(base):
        def tile(t):
            slot = slot_up(base + t)
            arrive("dn", t, slot)
            fetch_ahead("dn", n_dn, "gu", t + SLOTS - 1, base, slot_up)
            return slot

        def whole(slot, j, w):
            acc = product(slot, 0, top)
            for c in (0, 1):
                m = CHUNK[c]
                terms(acc[3 * start_row[c]:3 * start_row[c] + 3 * m], 0, start_row[c], m, j, w)

        slot = tile(0)
        terms(product(slot, 0, 3 * CHUNK[0]), 0, 0, CHUNK[0], 0, 0)
        send_terms(0, 0, 0, (0, CHUNK[0]))
        terms(product(slot, 3 * CHUNK[0], 3 * CHUNK[1]), 0, CHUNK[0], CHUNK[1], 0, 0)

        def send_first(j):
            @pl.when(j == 0)
            def _():
                send_terms(0, 0, 0, (CHUNK[0], CHUNK[1]))

            @pl.when(j > 0)
            def _():
                send_terms(0, j, 0)

        def body(j, carry):
            slot = tile(2 * j + 1)
            send_first(j)
            whole(slot, j, 1)
            slot = tile(2 * j + 2)
            send_terms(0, j, 1)
            whole(slot, j + 1, 0)
            return carry

        lax.fori_loop(0, pairs - 1, body, 0)
        slot = tile(n_dn - 1)
        send_terms(0, pairs - 1, 0)
        whole(slot, pairs - 1, 1)
        send_terms(0, pairs - 1, 1)

    def down_last(base):
        m = CHUNK[2]

        def peers(j, carry):
            for w in (0, 1):
                t = 2 * j + w
                slot = slot_up(base + t)
                arrive("dn", t, slot)
                fetch_ahead("dn", n_dn, None, t + SLOTS - 1, base, slot_up)
                if w == 1:
                    send_terms(1, j, 0)
                else:
                    @pl.when(j > 0)
                    def _():
                        send_terms(1, j - 1, 1)
                terms(product(slot, 0, 3 * m), 1, 0, m, j, w)
            return carry

        lax.fori_loop(0, pairs, peers, 0)

        for way in (LEFT, RIGHT):
            reduced(0, way, d, pairs)

        def mine(u, carry):
            j = pairs - 1 - u
            for w in (1, 0):
                s = 2 * u + 1 - w
                t = n_dn - 1 - s
                slot = slot_up(base + t)

                @pl.when(s >= SLOTS)
                def _():
                    arrive("dn", t, slot)

                @pl.when((s >= 1) & (s + SLOTS - 1 < n_dn))
                def _():
                    fetch("dn", t - (SLOTS - 1), slot_up(base + t + 1))

                if w == 1:
                    @pl.when(u == 0)
                    def _():
                        send_terms(1, pairs - 1, 1)

                    @pl.when(u < pairs - 1)
                    def _():
                        add_diag(1, u)
                else:
                    @pl.when(u < pairs - 1)
                    def _():
                        send_sum(1, u)
                own_rows(product(slot, top, rows), j, w)
            return carry

        lax.fori_loop(0, pairs, mine, 0)

    barrier = pltpu.get_barrier_semaphore()
    for way in (LEFT, RIGHT):
        pl.semaphore_signal(barrier, inc=1, device_id={"tp": peer[way]}, device_id_type=MESH)
    load = pltpu.make_async_copy(x, xown, xsem)
    load.start()
    fetch("gu", 0, slot_up(0))
    pl.semaphore_wait(barrier, 2)
    send_own(0)
    load.wait()
    for i in range(1, SLOTS - 1):
        fetch("gu", i, slot_up(i))

    def at(step, i, f, *ps):
        if isinstance(i, int):
            if i == step:
                f(*ps)
            return

        @pl.when(i == step)
        def _():
            f(*ps)

    def act0(i):
        at(3, i, send_own, 1)
        at(7, i, forward, 0)
        at(11, i, forward, 1)
        at(13, i, send_own, 2)

    def act1(k):
        at(2, k, send_own, 3)
        at(4, k, forward, 2)
        at(6, k, forward, 3)
        at(n_gu // 2, k, send_own, 4)

    def act2(k):
        at(2, k, send_own, 5)
        at(4, k, forward, 4)
        at(7, k, forward, 5)

    def act3(k):
        first = 2
        if isinstance(k, int):
            return

        @pl.when((k > first) & (k <= first + pairs))
        def _():
            send_sum(0, k - first - 1)

        @pl.when((k >= first) & (k < first + pairs))
        def _():
            add_diag(0, k - first)

    gate_up(xown, 0, rows, top, act0)
    gathered(0)
    gate_up_pairs(xc, 0, 0, "ug", 0, slot_back, None, act1, True)
    gathered(1)
    gate_up_pairs(xc, 1, 3 * CHUNK[0], "gu", 0, slot_up, "dn", act2, True)
    base = n_gu
    down_first(base)
    base += n_dn
    gathered(2)
    gate_up_pairs(xc, 2, 0, "gu", base, slot_up, "dn", act3, False)
    base += n_gu
    for way in (LEFT, RIGHT):
        drain(ag_s.at[way], 3 * rows // 2, way)
    down_last(base)

    add_diag(1, pairs - 1)
    finish(0)
    send_sum(1, pairs - 1)

    def finish_all(j, carry):
        finish(j)
        return carry

    lax.fori_loop(1, pairs, finish_all, 0)
    for way in (LEFT, RIGHT):
        for part in (0, 1):
            drain(rs_s.at[way, part], 3 * PART[part][1] // 2, way)


def solution(mesh):
    def step(x, w_gate, w_up, w_down):
        rows, d = x.shape
        ff = w_gate.shape[1]
        half, pairs = d // 2, d // 2 // TN
        any_spec = pl.BlockSpec(memory_space=pl.ANY)
        dma = pltpu.SemaphoreType.DMA
        return pl.pallas_call(
            _kernel,
            out_shape=pltpu.VMEM((rows, d), BF),
            in_specs=[any_spec] * 4,
            out_specs=pl.BlockSpec(memory_space=pltpu.VMEM),
            scratch_shapes=[
                pltpu.VMEM((rows, d), BF),
                pltpu.VMEM((3 * rows, d), BF),
                pltpu.VMEM((3 * PART[0][1] + rows, ff), BF),
                pltpu.VMEM((SLOTS, d, max(2 * TF, TN)), BF),
                pltpu.VMEM((rows, d), BF),
                pltpu.VMEM((2, rows, d), BF),
                pltpu.VMEM((2, rows, d), BF),
                pltpu.VMEM((max(PART[0][1], PART[1][1]), d), F32),
                pltpu.VMEM((PART[1][1], d), F32),
                dma(()),
                dma((SLOTS,)),
                dma((2,)),
                dma((2, len(PIECES))),
                dma((2, len(CHUNK))),
                dma((2, 2)),
                dma((2, 2, pairs)),
                dma((2, pairs + 1)),
            ],
            compiler_params=pltpu.CompilerParams(
                collective_id=0, has_side_effects=True, vmem_limit_bytes=64_600_000,
            ),
            cost_estimate=pl.CostEstimate(
                flops=6 * 4 * rows * d * ff, bytes_accessed=4 * 6 * d * ff, transcendentals=4 * rows * ff
            ),
        )(x, w_gate, w_up, w_down)

    return jax.shard_map(
        step,
        mesh=mesh,
        in_specs=(P(("dp", "tp"), None), P(None, "tp"), P(None, "tp"), P("tp", None)),
        out_specs=P(("dp", "tp"), None),
        check_vma=False,
    )
```
